32 devices in a mesh: dp: 4 (over y, x), expert: 8 (over z, core).
Axes of the slice: x: 2, y: 2, z: 4, core: 2. Of those that a mesh axis runs over, the one named last changes fastest.
Arguments:
- tokens: bfloat16 [8192, 2048], P(('dp', 'expert')), may hold values from -6 to 6
- expert_ids: int32 [8192, 8], P(('dp', 'expert')), may hold values from 0 to 15, all different within a row; in each aligned block of 256 rows (0 to 255, 256 to 511, ...) at most 160 rows name the same one
- route_probs: float32 [8192, 8], P(('dp', 'expert')), may hold values from 0.05 to 1
- w_gate_up: bfloat16 [16, 2048, 1536], P('expert', 'dp'), may hold values from -0.125 to 0.125
- w_down: bfloat16 [16, 768, 2048], P('expert', None, 'dp'), may hold values from -0.21875 to 0.21875
Outputs:
- moe_out: bfloat16 [8192, 2048], P(('dp', 'expert'))
The draws below stay inside these ranges and needn't reach their ends.
Inputs may be any that keep to these rules, and one draw needn't show every extreme that they name: `expert_ids`: each row names 8 different experts. Among the rows of one device no expert is named more than 160 times, and in every draw some expert is named exactly 160 times in some device's rows.
All inputs are finite; a program needn't handle non-finite values.
Results may differ from the reference program's by a relative error of at most 0.0057.
Values may be sent and summed in bfloat16 or wider, within the bound.
A program may use at most 128 MiB of HBM per device.

```python
import math
import jax
import jax.numpy as jnp
import numpy as np
from jax import lax

D = 2048
FF = 768
TOP = 8
TOK_DEV = 256
EXPERTS = 16
CAP = 160
TOKENS = 8192


def levels(rng, dims, split, smallest, high):
    gain = 1.0
    for axis_at, blocks in split:
        heights = jax.random.uniform(jax.random.fold_in(jax.random.fold_in(rng, 6), axis_at), (blocks,), jnp.float32, smallest / len(split), high / len(split))
        gain = gain * jnp.repeat(jnp.exp(heights), dims[axis_at] // blocks).reshape((-1,) + (1,) * (len(dims) - 1 - axis_at))
    return gain


def deal_out(stream_key, own, number, rows, count, top, limit, lean):
    sequence = jax.random.permutation(stream_key, count)
    packed, usual = shares(count, rows * top, limit, lean, True), shares(count, rows * top, limit, lean, False)
    places = jnp.arange(count)

    def named(sizes, offset_by):
        used = int((sizes > 0).sum())
        fixed = max(1, used // 4)
        shifted = fixed + (places - fixed + offset_by * (used - fixed)) % max(1, count - fixed)
        return jnp.zeros((count,), jnp.int32).at[sequence[jnp.where(places < fixed, places, shifted)]].set(jnp.asarray(sizes, jnp.int32))

    sizes = jnp.where(number % 4 == 0, named(packed, number // 4), named(usual, number - number // 4 - 1))
    mixed = jax.random.permutation(jax.random.fold_in(own, 3), count)
    source_of, taker = mixed[0:count // 2 * 2:2], mixed[1:count // 2 * 2:2]
    margin = jnp.minimum(sizes[source_of] - 1, limit - sizes[taker]) // 2
    margin = jnp.where((source_of == sequence[0]) | (taker == sequence[0]) | (sizes[taker] == 0), 0, jnp.maximum(margin, 0))
    shifted = jax.random.randint(jax.random.fold_in(own, 4), (count // 2,), 0, 1 << 20) % (margin + 1)
    sizes = sizes.at[source_of].add(-shifted).at[taker].add(shifted)
    labels = jnp.searchsorted(jnp.cumsum(sizes), jnp.arange(rows * top), side="right").astype(jnp.int32)
    listing = labels.reshape(top, rows).T
    listing = listing[jax.random.permutation(jax.random.fold_in(own, 1), rows)]
    offset_by = jax.random.randint(jax.random.fold_in(own, 2), (rows, 1), 0, top)
    return jnp.take_along_axis(listing, (jnp.arange(top)[None, :] + offset_by) % top, axis=1)


def shares(amount, total, reach, lean, full):
    loads = [(1 << 20) // math.isqrt(rank ** lean) + 1 for rank in range(1, amount + 1)]
    largest = reach if full else min(reach, max(-(-total // amount), total * loads[0] // sum(loads)))
    least = 1 if total - largest >= amount - 1 else 0
    given, rest = [largest] + [least] * (amount - 1), total - largest - least * (amount - 1)
    while rest > 0:
        movable = [i for i in range(1, amount) if given[i] < largest] or [i for i in range(1, amount) if given[i] < reach]
        mass, remaining = sum([loads[i] for i in movable]), rest
        for i in movable:
            more = min(reach - given[i], max(1, remaining * loads[i] // mass), rest)
            given[i] = given[i] + more
            rest = rest - more
    return np.array(given)


def normal_values(key, extent, width, reach, shards=(), kind=jnp.bfloat16):
    loudness = levels(key, extent, shards, -0.22, 0.18) if shards else 1.0
    array = jax.random.normal(key, extent, jnp.float32) * width * loudness
    return jnp.minimum(jnp.maximum(array, -reach), reach).astype(kind)


def setup_inputs(seed: int = 0) -> dict:
    arg_keys = jax.random.split(jax.random.key(seed), 6)
    tokens = normal_values(arg_keys[0], (TOKENS, D), 1.0, 6.0, ((0, 32),))
    expert_ids_keys = jax.random.split(jax.random.fold_in(arg_keys[1], 1), TOKENS // TOK_DEV)
    expert_ids_turns = jax.random.permutation(jax.random.fold_in(arg_keys[1], 3), TOKENS // TOK_DEV)
    expert_ids = jax.vmap(lambda own, number: deal_out(jax.random.fold_in(arg_keys[1], 2), own, number, TOK_DEV, EXPERTS, TOP, CAP, 1))(expert_ids_keys, expert_ids_turns).reshape((TOKENS, TOP))
    route_probs = jnp.clip(jnp.exp(math.log(1.0) - 2.9957323 * jax.random.uniform(arg_keys[2], (TOKENS, TOP), jnp.float32) ** levels(arg_keys[2], (TOKENS, TOP), ((0, 32),), -0.2, 0.2)), 0.05, 1.0)
    w_gate_up = normal_values(arg_keys[3], (EXPERTS, D, 2 * FF), D ** -0.5, 0.125, ((0, 8), (1, 4)))
    w_down = normal_values(arg_keys[4], (EXPERTS, FF, D), FF ** -0.5, 0.21875, ((0, 8), (2, 4)))
    return {"tokens": tokens, "expert_ids": expert_ids, "route_probs": route_probs, "w_gate_up": w_gate_up, "w_down": w_down}


def reference(tokens, expert_ids, route_probs, w_gate_up, w_down):
    experts = w_gate_up.shape[0]
    device_count = tokens.shape[0] // TOK_DEV
    slots_all = device_count * CAP
    weights = route_probs / jnp.sum(route_probs, axis=1, keepdims=True)
    blocks = expert_ids.reshape(device_count, TOK_DEV * TOP).astype(jnp.int32)
    onehot = (blocks[:, :, None] == jnp.arange(experts, dtype=jnp.int32)[None, None, :]).astype(jnp.int32)
    before = jnp.cumsum(onehot, axis=1) - onehot
    slot_of = jnp.sum(before * onehot, axis=2).astype(jnp.int32)
    device_of = jnp.arange(device_count, dtype=jnp.int32)[:, None]
    position = (blocks * slots_all + device_of * CAP + slot_of).reshape(-1).astype(jnp.int32)
    token_of = (device_of * TOK_DEV + jnp.arange(TOK_DEV * TOP, dtype=jnp.int32)[None, :] // TOP).reshape(-1).astype(jnp.int32)
    row_table = jnp.zeros((experts * slots_all,), jnp.int32).at[position].set(token_of).reshape(experts, slots_all)
    row_weight = jnp.zeros((experts * slots_all,), jnp.float32).at[position].set(weights.reshape(-1).astype(jnp.float32)).reshape(experts, slots_all)

    def expert_step(running, inputs):
        rows_index, rows_scale, gate_up, down = inputs
        rows_in = tokens[rows_index]
        joined = jnp.dot(rows_in, gate_up, preferred_element_type=jnp.float32)
        hidden = (jax.nn.silu(joined[:, :FF]) * joined[:, FF:]).astype(jnp.bfloat16)
        result = jnp.dot(hidden, down, preferred_element_type=jnp.float32).astype(jnp.bfloat16)
        result = lax.optimization_barrier(result).astype(jnp.float32)
        return running.at[rows_index].add(result * rows_scale[:, None]), None

    start_sum = jnp.zeros(tokens.shape, jnp.float32)
    summed, unused = lax.scan(expert_step, start_sum, (row_table, row_weight, w_gate_up, w_down))
    return summed.astype(jnp.bfloat16)
```

```python
import functools

import jax
import jax.numpy as jnp
from jax import lax
from jax.experimental import pallas as pl
from jax.experimental.pallas import tpu as pltpu
from jax.sharding import PartitionSpec as P

MESH = pl.DeviceIdType.MESH
LANES = 128


def xor(index, mask):
    width = 1
    while width <= mask:
        if mask & width:
            index = index + width * (1 - 2 * lax.rem(index // width, 2))
        width *= 2
    return index


def span(masks):
    out = [0]
    for m in masks:
        out = out + [m ^ s for s in out]
    return out


def powers(count):
    out, width = [], 1
    while width < count:
        out.append(width)
        width *= 2
    return out


class Gather:
    def __init__(self, orders, me, target, own, slot, send_sem, recv_sem):
        self.orders, self.me, self.target = orders, me, target
        self.own_ref, self.slot = own, slot
        self.send_sem, self.recv_sem = send_sem, recv_sem
        self.last = len(orders[0]) - 1
        self.taken = set()

    def _copy(self, half, g, s):
        dst = self.slot(xor(self.me, s), half)
        return pltpu.make_async_remote_copy(
            src_ref=self.own_ref(half) if s == 0 else dst,
            dst_ref=dst,
            send_sem=self.send_sem.at[half, g ^ s],
            recv_sem=self.recv_sem.at[half, g ^ s],
            device_id=self.target(xor(self.me, g)),
            device_id_type=MESH,
        )

    def own(self, stage):
        for half, order in enumerate(self.orders):
            self._copy(half, order[stage], 0).start()

    def relay(self, stage):
        for half, order in enumerate(self.orders):
            for s in span(order[:stage])[1:]:
                self._copy(half, order[stage], s).start()

    def take(self, half, off):
        if (half, off) in self.taken:
            return
        self.taken.add((half, off))
        ref = self.slot(xor(self.me, off), half)
        pltpu.make_async_remote_copy(
            src_ref=ref,
            dst_ref=ref,
            send_sem=self.send_sem.at[half, off],
            recv_sem=self.recv_sem.at[half, off],
            device_id=self.target(xor(self.me, off)),
            device_id_type=MESH,
        ).wait_recv()

    def wait(self, stage):
        for half, order in enumerate(self.orders):
            for s in span(order[:stage]):
                self.take(half, order[stage] ^ s)

    def forward(self):
        for stage in range(1, self.last + 1):
            self.wait(stage - 1)
            self.relay(stage)

    def drain(self):
        for half, order in enumerate(self.orders):
            for stage, g in enumerate(order):
                for s in span(order[:stage]):
                    self._copy(half, g, s).wait_send()


def kernel(
    dps, owners,
    tok_in, ids_in, prob_in, gu_in, dn_in, out,
    tok, share_out, share, gu, dn, hid, near, got,
    tok_s, tok_r, share_s, share_r, gu_s, gu_r, gus_s, gus_r, dn_s, dn_r, dns_s, dns_r,
    near_s, near_r, out_s, out_r, loc, gu_l, dn_l, fin,
):
    dp, ex = lax.axis_index("dp"), lax.axis_index("expert")
    chips, pairs = owners // 2, owners // 4
    chip, core = ex // 2, lax.rem(ex, 2)
    pair, side = chip // 2, lax.rem(chip, 2)
    local, depth, both = gu_in.shape
    ff, cols = dn_in.shape[1:]
    rows, width = tok_in.shape
    count = 2 * local
    tiles, strips = ff // LANES, cols // LANES
    units = local * tiles
    mine = local * ff

    dp_masks = powers(dps)
    chip_masks = [2 * (2 * w - 1) for w in powers(chips)]

    barrier = pltpu.get_barrier_semaphore()
    peers = [(xor(dp, m), ex) for m in dp_masks] + [(dp, xor(ex, 1))]
    peers += [(dp, xor(ex, 2 * r)) for r in range(1, chips)]
    for peer in peers:
        pl.semaphore_signal(barrier, inc=1, device_id=peer, device_id_type=MESH)

    def on_expert(index):
        return (dp, index)

    def on_dp(index):
        return (index, ex)

    sibling = (dp, xor(ex, 1))

    def stage_unit(u):
        e, j = u // tiles, lax.rem(u, tiles)
        at = pl.ds(pl.multiple_of(dp * depth, depth), depth)
        return [
            pltpu.make_async_copy(
                gu_in.at[e, :, pl.ds(pl.multiple_of(k * ff + j * LANES, LANES), LANES)],
                gu.at[u, at, pl.ds(k * LANES, LANES)],
                gu_l.at[u, k],
            )
            for k in range(2)
        ]

    def stage_strip(s):
        return [
            pltpu.make_async_copy(
                dn_in.at[e, :, pl.ds(s * LANES, LANES)], dn.at[s, dp, pl.ds(e * ff, ff)], dn_l.at[s, e]
            )
            for e in range(local)
        ]

    own_tok = pltpu.make_async_copy(tok_in, tok.at[pair, side], loc.at[0])

    @functools.partial(lax.fori_loop, 0, units, init_val=0)
    def _(u, carry):
        for copy in stage_unit(u):
            copy.start()
        return carry

    own_tok.start()
    for s in range(strips):
        for copy in stage_strip(s):
            copy.start()

    half_rows, half_depth, half_mine = rows // 2, depth // 2, mine // 2
    tokens = Gather(
        [chip_masks, chip_masks[::-1]], ex, on_expert,
        lambda h: tok_in.at[pl.ds(h * half_rows, half_rows)],
        lambda b, h: tok.at[b // 4, lax.rem(b // 2, 2), pl.ds(h * half_rows, half_rows)],
        tok_s, tok_r,
    )

    def up(u):
        def slot(b, h):
            return gu.at[u, pl.ds(pl.multiple_of(b * depth + h * half_depth, half_depth), half_depth)]

        return Gather(
            [dp_masks, dp_masks[::-1]], dp, on_dp, lambda h: slot(dp, h), slot, gu_s.at[u], gu_r.at[u]
        )

    def down(s):
        def slot(b, h):
            return dn.at[s, b, pl.ds(h * half_mine, half_mine)]

        return Gather(
            [dp_masks, dp_masks[::-1]], dp, on_dp, lambda h: slot(dp, h), slot, dn_s.at[s], dn_r.at[s]
        )

    last = len(dp_masks) - 1

    def up_own(u):
        for copy in stage_unit(u):
            copy.wait()
        g = up(u)
        for stage in range(last + 1):
            g.own(stage)

    def down_own(s):
        g = down(s)
        for stage in range(last + 1):
            g.own(stage)

    def up_sib(u):
        return pltpu.make_async_remote_copy(
            src_ref=gu.at[u], dst_ref=gu.at[units + u], send_sem=gus_s.at[u], recv_sem=gus_r.at[u],
            device_id=sibling, device_id_type=MESH,
        )

    def down_sib(s, b, m):
        return pltpu.make_async_remote_copy(
            src_ref=dn.at[s, b, pl.ds(0, mine)], dst_ref=dn.at[s, b, pl.ds(mine, mine)],
            send_sem=dns_s.at[s, m], recv_sem=dns_r.at[s, m],
            device_id=sibling, device_id_type=MESH,
        )

    pl.semaphore_wait(barrier, len(peers))
    for stage in range(tokens.last + 1):
        tokens.own(stage)
    up_own(0)
    up_own(1)

    prob = prob_in[...]
    weight = prob / jnp.sum(prob, axis=0, keepdims=True)
    ids = ids_in[...]
    pad = share_out.shape[1] - count
    for c in range(chips):
        lines = [
            jnp.sum(
                jnp.where(ids == c * count + lax.rem(core * local + k, count), weight, 0.0), axis=0, keepdims=True
            )
            for k in range(count)
        ]
        if pad:
            lines.append(jnp.zeros((pad, rows), jnp.float32))
        share_out[c] = jnp.concatenate(lines, axis=0)

    def to_chip(r):
        other = xor(ex, 2 * r)
        return pltpu.make_async_remote_copy(
            src_ref=share_out.at[other // 2], dst_ref=share.at[chip],
            send_sem=share_s.at[r], recv_sem=share_r.at[r],
            device_id=on_expert(other), device_id_type=MESH,
        )

    for r in range(1, chips):
        to_chip(r).start()

    fold = 2 if pairs <= 2 else 1

    def hidden(p, v):
        def body(i, carry):
            x = tok[p, pl.ds(i * fold, fold)].reshape(fold * rows, width)
            ab = jnp.dot(x, gu[v], preferred_element_type=jnp.float32)
            a, b = ab[:, :LANES], ab[:, LANES:]
            by = jnp.concatenate([jnp.transpose(share[2 * p + i * fold + k]) for k in range(fold)], axis=0)
            lane = lax.broadcasted_iota(jnp.int32, by.shape, 1)
            by = jnp.sum(jnp.where(lane == v // tiles, by, 0.0), axis=1, keepdims=True)
            at = pl.ds(pl.multiple_of(i * fold * rows, fold * rows), fold * rows)
            hid[p, at, pl.ds(pl.multiple_of(v * LANES, LANES), LANES)] = (
                a / (1.0 + jnp.exp(-a)) * b * by
            ).astype(hid.dtype)
            return carry

        if fold == 2:
            body(0, 0)
        else:
            lax.fori_loop(0, 2, body, 0)

    def relay_step(u, ahead):
        @pl.when(u + ahead < units)
        def _():
            up_own(u + ahead)

        @pl.when(u + 1 < units)
        def _():
            up(u + 1).forward()

        @pl.when(u + 2 == units)
        def _():
            down_own(0)

    begin, early = units // 3, 2 * units // 3

    up(0).forward()
    for u in range(begin):
        relay_step(u, 2)
        if u == begin // 2:
            tokens.forward()
        up(u).wait(last)
        up_sib(u).start()

    own_tok.wait()
    for half in range(2):
        tokens.take(half, 2)
    share_own = share_out[chip]
    share[chip] = share_own
    for r in range(1, chips):
        pltpu.make_async_remote_copy(
            src_ref=share_out.at[0], dst_ref=share.at[xor(ex, 2 * r) // 2],
            send_sem=share_s.at[r], recv_sem=share_r.at[r],
            device_id=on_expert(xor(ex, 2 * r)), device_id_type=MESH,
        ).wait_recv()

    def both_of(v):
        hidden(pair, v)
        up_sib(v).wait_recv()
        hidden(pair, units + v)

    def phase_one(u, carry):
        relay_step(u, 2)
        share_of(u - begin, begin, early - begin, both_of)
        up(u).wait(last)
        up_sib(u).start()
        both_of(u)
        return carry

    def share_of(i, total, parts, body):
        each = -(-total // parts)

        def one(n, carry):
            @pl.when(i * each + n < total)
            def _():
                body(i * each + n)

            return carry

        lax.fori_loop(0, each, one, 0)

    lax.fori_loop(begin, early, phase_one, 0)

    for copy in [c for s in range(strips) for c in stage_strip(s)]:
        copy.wait()
    for s in range(strips):
        down_sib(s, dp, 0).start()
    tokens.wait(tokens.last)
    for stage in range(tokens.last):
        tokens.wait(stage)

    def others_of(v):
        for r in range(1, pairs):
            hidden(xor(pair, r), v)
            hidden(xor(pair, r), units + v)

    def phase_two(u, carry):
        relay_step(u, 2)
        share_of(u - early, early, units - early, others_of)
        up(u).wait(last)
        up_sib(u).start()

        def every(p, v):
            hidden(p, v)
            return v

        lax.fori_loop(0, pairs, every, u)
        up_sib(u).wait_recv()
        lax.fori_loop(0, pairs, every, units + u)
        return carry

    lax.fori_loop(early, units, phase_two, 0)

    tokens.drain()

    steps = [(s, 0) for s in range(strips)] + [(s, m) for s in range(strips) for m in range(1, dps)]

    def where(k):
        s, m = steps[k]
        return pl.ds(pl.multiple_of(xor(dp, m) * cols + s * LANES, LANES), LANES)

    def to_near(k):
        at = where(k)
        return pltpu.make_async_remote_copy(
            src_ref=tok.at[:, 1 - side, :, at], dst_ref=near.at[:, :, at],
            send_sem=near_s.at[k], recv_sem=near_r.at[k],
            device_id=on_expert(xor(ex, 2)), device_id_type=MESH,
        )

    def to_home(k, r):
        at = where(k)
        return pltpu.make_async_remote_copy(
            src_ref=tok.at[xor(pair, r), side, :, at], dst_ref=got.at[r - 1, :, at],
            send_sem=out_s.at[k, r], recv_sem=out_r.at[k, r],
            device_id=on_expert(xor(ex, 4 * r)), device_id_type=MESH,
        )

    def to_out(k):
        at = where(k)
        return pltpu.make_async_copy(tok.at[pair, side, :, at], out.at[:, at], fin.at[k])

    def partial(k):
        s, m = steps[k]
        b, at = xor(dp, m), where(k)

        def body(p, carry):
            total = jnp.dot(hid[p], dn[s, b], preferred_element_type=jnp.float32)
            tok[p, :, :, at] = total.astype(tok.dtype).reshape(2, rows, LANES)
            return carry

        lax.fori_loop(0, pairs, body, 0)
        to_near(k).start()

    def pass_on(k):
        at = where(k)
        to_near(k).wait_recv()
        for r in range(1, pairs):
            p = xor(pair, r)
            tok[p, side, :, at] = (
                tok[p, side, :, at].astype(jnp.float32) + near[p, :, at].astype(jnp.float32)
            ).astype(tok.dtype)
            to_home(k, r).start()

    def finish(k):
        at = where(k)
        total = tok[pair, side, :, at].astype(jnp.float32) + near[pair, :, at].astype(jnp.float32)
        for r in range(1, pairs):
            to_home(k, r).wait_recv()
            total = total + got[r - 1, :, at].astype(jnp.float32)
        tok[pair, side, :, at] = total.astype(tok.dtype)
        to_out(k).start()

    lag = 2

    def advance(k):
        if k < len(steps):
            partial(k)
        if 0 <= k - lag < len(steps):
            pass_on(k - lag)
        if 0 <= k - 2 * lag < len(steps):
            finish(k - 2 * lag)

    if strips > 1:
        down_own(1)
    for s in range(strips):
        down_sib(s, dp, 0).wait_recv()
        advance(s)
        if s == 0:
            down(0).forward()
        if s == strips // 2:
            if strips > 2:
                down_own(2)
            if strips > 1:
                down(1).forward()
    k = strips
    for s in range(strips):
        down(s).wait(last)
        for m in range(1, dps):
            down_sib(s, xor(dp, m), m).start()
        for m in range(1, dps):
            down_sib(s, xor(dp, m), m).wait_recv()
            advance(k)
            k += 1
            if m == 1:
                if s + 3 < strips:
                    down_own(s + 3)
                if s + 2 < strips:
                    down(s + 2).forward()
    while k < len(steps) + 2 * lag:
        advance(k)
        k += 1

    def drained(u, carry):
        up(u).drain()
        up_sib(u).wait_send()
        return carry

    lax.fori_loop(0, units, drained, 0)
    for s in range(strips):
        down(s).drain()
        for m in range(dps):
            down_sib(s, xor(dp, m), m).wait_send()
    for r in range(1, chips):
        to_chip(r).wait_send()
    for k in range(len(steps)):
        to_near(k).wait_send()
        for r in range(1, pairs):
            to_home(k, r).wait_send()
        to_out(k).wait()


def shards(tokens, expert_ids, route_probs, w_gate_up, w_down):
    dps, owners = lax.axis_size("dp"), lax.axis_size("expert")
    chips, pairs = owners // 2, owners // 4
    local, depth, both = w_gate_up.shape
    rows, width = tokens.shape
    ff, cols = w_down.shape[1:]
    count = 2 * local
    lines = count + -count % 8
    tiles, strips = ff // LANES, cols // LANES
    units, steps = local * tiles, strips * dps
    any_ = pl.BlockSpec(memory_space=pl.ANY)
    vmem = pl.BlockSpec(memory_space=pltpu.VMEM)
    dma = pltpu.SemaphoreType.DMA
    bf16, f32 = jnp.bfloat16, jnp.float32
    return pl.pallas_call(
        functools.partial(kernel, dps, owners),
        out_shape=jax.ShapeDtypeStruct((rows, width), bf16),
        in_specs=[any_, vmem, vmem, any_, any_],
        out_specs=any_,
        scratch_shapes=[
            pltpu.VMEM((pairs, 2, rows, width), bf16),
            pltpu.VMEM((chips, lines, rows), f32),
            pltpu.VMEM((chips, lines, rows), f32),
            pltpu.VMEM((2 * units, dps * depth, 2 * LANES), bf16),
            pltpu.VMEM((strips, dps, count * ff, LANES), bf16),
            pltpu.VMEM((pairs, 2 * rows, count * ff), bf16),
            pltpu.VMEM((pairs, rows, width), bf16),
            pltpu.VMEM((max(pairs - 1, 1), rows, width), bf16),
            dma((2, owners)), dma((2, owners)),
            dma((chips,)), dma((chips,)),
            dma((units, 2, dps)), dma((units, 2, dps)),
            dma((units,)), dma((units,)),
            dma((strips, 2, dps)), dma((strips, 2, dps)),
            dma((strips, dps)), dma((strips, dps)),
            dma((steps,)), dma((steps,)),
            dma((steps, pairs)), dma((steps, pairs)),
            dma((1,)), dma((units, 2)), dma((strips, local)), dma((steps,)),
        ],
        compiler_params=pltpu.CompilerParams(
            collective_id=0, has_side_effects=True, vmem_limit_bytes=67043328
        ),
    )(tokens, expert_ids.T, route_probs.T, w_gate_up, w_down)


def solution(mesh):
    return jax.shard_map(
        shards,
        mesh=mesh,
        in_specs=(
            P(("dp", "expert"), None),
            P(("dp", "expert"), None),
            P(("dp", "expert"), None),
            P("expert", "dp", None),
            P("expert", None, "dp"),
        ),
        out_specs=P(("dp", "expert"), None),
        check_vma=False,
    )
```

```python
import functools

import jax
import jax.numpy as jnp
from jax import lax
from jax.experimental import pallas as pl
from jax.experimental.pallas import tpu as pltpu
from jax.sharding import PartitionSpec as P

MESH = pl.DeviceIdType.MESH
LANES = 128


def xor(index, mask):
    width = 1
    while width <= mask:
        if mask & width:
            index = index + width * (1 - 2 * lax.rem(index // width, 2))
        width *= 2
    return index


def span(masks):
    out = [0]
    for m in masks:
        out = out + [m ^ s for s in out]
    return out


def powers(count):
    out, width = [], 1
    while width < count:
        out.append(width)
        width *= 2
    return out


class Gather:
    def __init__(self, orders, me, target, own, slot, send_sem, recv_sem):
        self.orders, self.me, self.target = orders, me, target
        self.own_ref, self.slot = own, slot
        self.send_sem, self.recv_sem = send_sem, recv_sem
        self.last = len(orders[0]) - 1
        self.taken = set()

    def _copy(self, half, g, s):
        dst = self.slot(xor(self.me, s), half)
        return pltpu.make_async_remote_copy(
            src_ref=self.own_ref(half) if s == 0 else dst,
            dst_ref=dst,
            send_sem=self.send_sem.at[half, g ^ s],
            recv_sem=self.recv_sem.at[half, g ^ s],
            device_id=self.target(xor(self.me, g)),
            device_id_type=MESH,
        )

    def own(self, stage, halves=(0, 1)):
        for half in halves:
            self._copy(half, self.orders[half][stage], 0).start()

    def relay(self, stage, halves=(0, 1)):
        for half in halves:
            order = self.orders[half]
            for s in span(order[:stage])[1:]:
                self._copy(half, order[stage], s).start()

    def take(self, half, off):
        if (half, off) in self.taken:
            return
        self.taken.add((half, off))
        ref = self.slot(xor(self.me, off), half)
        pltpu.make_async_remote_copy(
            src_ref=ref,
            dst_ref=ref,
            send_sem=self.send_sem.at[half, off],
            recv_sem=self.recv_sem.at[half, off],
            device_id=self.target(xor(self.me, off)),
            device_id_type=MESH,
        ).wait_recv()

    def wait(self, stage, halves=(0, 1)):
        for half in halves:
            order = self.orders[half]
            for s in span(order[:stage]):
                self.take(half, order[stage] ^ s)

    def forward(self, halves=(0, 1)):
        for stage in range(1, self.last + 1):
            self.wait(stage - 1, halves)
            self.relay(stage, halves)

    def drain(self):
        for half, order in enumerate(self.orders):
            for stage, g in enumerate(order):
                for s in span(order[:stage]):
                    self._copy(half, g, s).wait_send()


def kernel(
    dps, owners,
    tok_in, ids_in, prob_in, gu_in, dn_in, out,
    tok, share_out, share, gu, dn, hid, near, got,
    tok_s, tok_r, share_s, share_r, gu_s, gu_r, gus_s, gus_r, dn_s, dn_r, dns_s, dns_r,
    near_s, near_r, out_s, out_r, loc, gu_l, dn_l, fin,
):
    dp, ex = lax.axis_index("dp"), lax.axis_index("expert")
    chips, pairs = owners // 2, owners // 4
    chip, core = ex // 2, lax.rem(ex, 2)
    pair, side = chip // 2, lax.rem(chip, 2)
    local, depth, both = gu_in.shape
    ff, cols = dn_in.shape[1:]
    rows, width = tok_in.shape
    count = 2 * local
    tiles, strips = ff // LANES, cols // LANES
    units = local * tiles
    mine = local * ff

    dp_masks = powers(dps)
    chip_masks = [2 * (2 * w - 1) for w in powers(chips)]

    barrier = pltpu.get_barrier_semaphore()
    peers = [(xor(dp, m), ex) for m in dp_masks] + [(dp, xor(ex, 1))]
    peers += [(dp, xor(ex, 2 * r)) for r in range(1, chips)]
    for peer in peers:
        pl.semaphore_signal(barrier, inc=1, device_id=peer, device_id_type=MESH)

    def on_expert(index):
        return (dp, index)

    def on_dp(index):
        return (index, ex)

    sibling = (dp, xor(ex, 1))

    def stage_unit(u):
        e, j = u // tiles, lax.rem(u, tiles)
        at = pl.ds(pl.multiple_of(dp * depth, depth), depth)
        return [
            pltpu.make_async_copy(
                gu_in.at[e, :, pl.ds(pl.multiple_of(k * ff + j * LANES, LANES), LANES)],
                gu.at[u, at, pl.ds(k * LANES, LANES)],
                gu_l.at[u, k],
            )
            for k in range(2)
        ]

    def stage_strip(s):
        return [
            pltpu.make_async_copy(
                dn_in.at[e, :, pl.ds(s * LANES, LANES)], dn.at[s, dp, pl.ds(e * ff, ff)], dn_l.at[s, e]
            )
            for e in range(local)
        ]

    own_tok = pltpu.make_async_copy(tok_in, tok.at[pair, side], loc.at[0])

    @functools.partial(lax.fori_loop, 0, units, init_val=0)
    def _(u, carry):
        for copy in stage_unit(u):
            copy.start()
        return carry

    own_tok.start()
    for s in range(strips):
        for copy in stage_strip(s):
            copy.start()

    half_rows, half_depth, half_mine = rows // 2, depth // 2, mine // 2
    tokens = Gather(
        [chip_masks, chip_masks[::-1]], ex, on_expert,
        lambda h: tok_in.at[pl.ds(h * half_rows, half_rows)],
        lambda b, h: tok.at[b // 4, lax.rem(b // 2, 2), pl.ds(h * half_rows, half_rows)],
        tok_s, tok_r,
    )

    def up(u):
        def slot(b, h):
            return gu.at[u, pl.ds(pl.multiple_of(b * depth + h * half_depth, half_depth), half_depth)]

        return Gather(
            [dp_masks, dp_masks[::-1]], dp, on_dp, lambda h: slot(dp, h), slot, gu_s.at[u], gu_r.at[u]
        )

    def down(s):
        def slot(b, h):
            return dn.at[s, b, pl.ds(h * half_mine, half_mine)]

        return Gather(
            [dp_masks, dp_masks[::-1]], dp, on_dp, lambda h: slot(dp, h), slot, dn_s.at[s], dn_r.at[s]
        )

    last = len(dp_masks) - 1

    def up_own(u):
        for copy in stage_unit(u):
            copy.wait()
        g = up(u)
        for stage in range(last + 1):
            g.own(stage)

    def down_own(s):
        g = down(s)
        for stage in range(last + 1):
            g.own(stage)

    def up_sib(u):
        return pltpu.make_async_remote_copy(
            src_ref=gu.at[u], dst_ref=gu.at[units + u], send_sem=gus_s.at[u], recv_sem=gus_r.at[u],
            device_id=sibling, device_id_type=MESH,
        )

    def down_sib(s, b, m):
        return pltpu.make_async_remote_copy(
            src_ref=dn.at[s, b, pl.ds(0, mine)], dst_ref=dn.at[s, b, pl.ds(mine, mine)],
            send_sem=dns_s.at[s, m], recv_sem=dns_r.at[s, m],
            device_id=sibling, device_id_type=MESH,
        )

    pl.semaphore_wait(barrier, len(peers))
    for stage in range(tokens.last + 1):
        tokens.own(stage)
    up_own(0)
    up_own(1)

    prob = prob_in[...]
    weight = prob / jnp.sum(prob, axis=0, keepdims=True)
    ids = ids_in[...]
    pad = share_out.shape[1] - count
    for c in range(chips):
        lines = [
            jnp.sum(
                jnp.where(ids == c * count + lax.rem(core * local + k, count), weight, 0.0), axis=0, keepdims=True
            )
            for k in range(count)
        ]
        if pad:
            lines.append(jnp.zeros((pad, rows), jnp.float32))
        share_out[c] = jnp.concatenate(lines, axis=0)

    def to_chip(r):
        other = xor(ex, 2 * r)
        return pltpu.make_async_remote_copy(
            src_ref=share_out.at[other // 2], dst_ref=share.at[chip],
            send_sem=share_s.at[r], recv_sem=share_r.at[r],
            device_id=on_expert(other), device_id_type=MESH,
        )

    for r in range(1, chips):
        to_chip(r).start()

    fold = 2 if pairs <= 2 else 1

    def hidden(p, v):
        def body(i, carry):
            x = tok[p, pl.ds(i * fold, fold)].reshape(fold * rows, width)
            ab = jnp.dot(x, gu[v], preferred_element_type=jnp.float32)
            a, b = ab[:, :LANES], ab[:, LANES:]
            by = jnp.concatenate([jnp.transpose(share[2 * p + i * fold + k]) for k in range(fold)], axis=0)
            lane = lax.broadcasted_iota(jnp.int32, by.shape, 1)
            by = jnp.sum(jnp.where(lane == v // tiles, by, 0.0), axis=1, keepdims=True)
            at = pl.ds(pl.multiple_of(i * fold * rows, fold * rows), fold * rows)
            hid[p, at, pl.ds(pl.multiple_of(v * LANES, LANES), LANES)] = (
                a / (1.0 + jnp.exp(-a)) * b * by
            ).astype(hid.dtype)
            return carry

        if fold == 2:
            body(0, 0)
        else:
            lax.fori_loop(0, 2, body, 0)

    def relay_step(u, ahead):
        @pl.when(u + ahead < units)
        def _():
            up_own(u + ahead)

        @pl.when(u + 1 < units)
        def _():
            up(u + 1).forward()

        @pl.when(u + 2 == units)
        def _():
            down_own(0)

    begin, early = 5 * units // 12, 2 * units // 3

    up(0).forward()
    for u in range(begin):
        relay_step(u, 2)
        if u == 1:
            tokens.forward((0,))
        if u == 3:
            tokens.forward((1,))
        up(u).wait(last)
        up_sib(u).start()

    own_tok.wait()
    for half in range(2):
        tokens.take(half, 2)
    share_own = share_out[chip]
    share[chip] = share_own
    for r in range(1, chips):
        pltpu.make_async_remote_copy(
            src_ref=share_out.at[0], dst_ref=share.at[xor(ex, 2 * r) // 2],
            send_sem=share_s.at[r], recv_sem=share_r.at[r],
            device_id=on_expert(xor(ex, 2 * r)), device_id_type=MESH,
        ).wait_recv()

    def both_of(v):
        hidden(pair, v)
        up_sib(v).wait_recv()
        hidden(pair, units + v)

    def phase_one(u, carry):
        relay_step(u, 2)
        share_of(u - begin, begin, early - begin, both_of)
        up(u).wait(last)
        up_sib(u).start()
        both_of(u)
        return carry

    def share_of(i, total, parts, body):
        each = -(-total // parts)

        def one(n, carry):
            @pl.when(i * each + n < total)
            def _():
                body(i * each + n)

            return carry

        lax.fori_loop(0, each, one, 0)

    lax.fori_loop(begin, early, phase_one, 0)

    for copy in [c for s in range(strips) for c in stage_strip(s)]:
        copy.wait()
    for s in range(strips):
        down_sib(s, dp, 0).start()
    tokens.wait(tokens.last)
    for stage in range(tokens.last):
        tokens.wait(stage)

    def others_of(v):
        for r in range(1, pairs):
            hidden(xor(pair, r), v)
            hidden(xor(pair, r), units + v)

    def phase_two(u, carry):
        relay_step(u, 2)
        share_of(u - early, early, units - early, others_of)
        up(u).wait(last)
        up_sib(u).start()

        def every(p, v):
            hidden(p, v)
            return v

        lax.fori_loop(0, pairs, every, u)
        up_sib(u).wait_recv()
        lax.fori_loop(0, pairs, every, units + u)
        return carry

    lax.fori_loop(early, units, phase_two, 0)

    tokens.drain()

    steps = [(s, 0) for s in range(strips)] + [(s, m) for s in range(strips) for m in range(1, dps)]

    def where(k):
        s, m = steps[k]
        return pl.ds(pl.multiple_of(xor(dp, m) * cols + s * LANES, LANES), LANES)

    def to_near(k):
        at = where(k)
        return pltpu.make_async_remote_copy(
            src_ref=tok.at[:, 1 - side, :, at], dst_ref=near.at[:, :, at],
            send_sem=near_s.at[k], recv_sem=near_r.at[k],
            device_id=on_expert(xor(ex, 2)), device_id_type=MESH,
        )

    def to_home(k, r):
        at = where(k)
        return pltpu.make_async_remote_copy(
            src_ref=tok.at[xor(pair, r), side, :, at], dst_ref=got.at[r - 1, :, at],
            send_sem=out_s.at[k, r], recv_sem=out_r.at[k, r],
            device_id=on_expert(xor(ex, 4 * r)), device_id_type=MESH,
        )

    def to_out(k):
        at = where(k)
        return pltpu.make_async_copy(tok.at[pair, side, :, at], out.at[:, at], fin.at[k])

    def partial(k):
        s, m = steps[k]
        b, at = xor(dp, m), where(k)

        def body(p, carry):
            total = jnp.dot(hid[p], dn[s, b], preferred_element_type=jnp.float32)
            tok[p, :, :, at] = total.astype(tok.dtype).reshape(2, rows, LANES)
            return carry

        lax.fori_loop(0, pairs, body, 0)
        to_near(k).start()

    def pass_on(k):
        at = where(k)
        to_near(k).wait_recv()
        for r in range(1, pairs):
            p = xor(pair, r)
            tok[p, side, :, at] = (
                tok[p, side, :, at].astype(jnp.float32) + near[p, :, at].astype(jnp.float32)
            ).astype(tok.dtype)
            to_home(k, r).start()

    def finish(k):
        at = where(k)
        total = tok[pair, side, :, at].astype(jnp.float32) + near[pair, :, at].astype(jnp.float32)
        for r in range(1, pairs):
            to_home(k, r).wait_recv()
            total = total + got[r - 1, :, at].astype(jnp.float32)
        tok[pair, side, :, at] = total.astype(tok.dtype)
        to_out(k).start()

    lag = 2

    def advance(k):
        if k < len(steps):
            partial(k)
        if 0 <= k - lag < len(steps):
            pass_on(k - lag)
        if 0 <= k - 2 * lag < len(steps):
            finish(k - 2 * lag)

    def down_next(s):
        if s < strips:
            down(s).forward()
        if s + 1 < strips:
            down_own(s + 1)

    for s in range(strips):
        down_sib(s, dp, 0).wait_recv()
        advance(s)
        if s == 0:
            down_next(0)
    down_next(1)
    k = strips
    for s in range(strips):
        down(s).wait(last)
        for m in range(1, dps):
            down_sib(s, xor(dp, m), m).start()
        for m in range(1, dps):
            down_sib(s, xor(dp, m), m).wait_recv()
            advance(k)
            k += 1
        down_next(s + 2)
    while k < len(steps) + 2 * lag:
        advance(k)
        k += 1

    def drained(u, carry):
        up(u).drain()
        up_sib(u).wait_send()
        return carry

    lax.fori_loop(0, units, drained, 0)
    for s in range(strips):
        down(s).drain()
        for m in range(dps):
            down_sib(s, xor(dp, m), m).wait_send()
    for r in range(1, chips):
        to_chip(r).wait_send()
    for k in range(len(steps)):
        to_near(k).wait_send()
        for r in range(1, pairs):
            to_home(k, r).wait_send()
        to_out(k).wait()


def shards(tokens, expert_ids, route_probs, w_gate_up, w_down):
    dps, owners = lax.axis_size("dp"), lax.axis_size("expert")
    chips, pairs = owners // 2, owners // 4
    local, depth, both = w_gate_up.shape
    rows, width = tokens.shape
    ff, cols = w_down.shape[1:]
    count = 2 * local
    lines = count + -count % 8
    tiles, strips = ff // LANES, cols // LANES
    units, steps = local * tiles, strips * dps
    any_ = pl.BlockSpec(memory_space=pl.ANY)
    vmem = pl.BlockSpec(memory_space=pltpu.VMEM)
    dma = pltpu.SemaphoreType.DMA
    bf16, f32 = jnp.bfloat16, jnp.float32
    return pl.pallas_call(
        functools.partial(kernel, dps, owners),
        out_shape=jax.ShapeDtypeStruct((rows, width), bf16),
        in_specs=[any_, vmem, vmem, any_, any_],
        out_specs=any_,
        scratch_shapes=[
            pltpu.VMEM((pairs, 2, rows, width), bf16),
            pltpu.VMEM((chips, lines, rows), f32),
            pltpu.VMEM((chips, lines, rows), f32),
            pltpu.VMEM((2 * units, dps * depth, 2 * LANES), bf16),
            pltpu.VMEM((strips, dps, count * ff, LANES), bf16),
            pltpu.VMEM((pairs, 2 * rows, count * ff), bf16),
            pltpu.VMEM((pairs, rows, width), bf16),
            pltpu.VMEM((max(pairs - 1, 1), rows, width), bf16),
            dma((2, owners)), dma((2, owners)),
            dma((chips,)), dma((chips,)),
            dma((units, 2, dps)), dma((units, 2, dps)),
            dma((units,)), dma((units,)),
            dma((strips, 2, dps)), dma((strips, 2, dps)),
            dma((strips, dps)), dma((strips, dps)),
            dma((steps,)), dma((steps,)),
            dma((steps, pairs)), dma((steps, pairs)),
            dma((1,)), dma((units, 2)), dma((strips, local)), dma((steps,)),
        ],
        compiler_params=pltpu.CompilerParams(
            collective_id=0, has_side_effects=True, vmem_limit_bytes=67043328
        ),
    )(tokens, expert_ids.T, route_probs.T, w_gate_up, w_down)


def solution(mesh):
    return jax.shard_map(
        shards,
        mesh=mesh,
        in_specs=(
            P(("dp", "expert"), None),
            P(("dp", "expert"), None),
            P(("dp", "expert"), None),
            P("expert", "dp", None),
            P("expert", None, "dp"),
        ),
        out_specs=P(("dp", "expert"), None),
        check_vma=False,
    )
```
